32 devices in a mesh: wide: 8 (over y, x, core), narrow: 4 (over z).
Axes of the slice: x: 2, y: 2, z: 4, core: 2. Of those that a mesh axis runs over, the one named last changes fastest.
Arguments:
- left: bfloat16 [32, 32, 256], P('narrow', None, 'wide'), may hold values from -6 to 6
- right: bfloat16 [32, 32, 256], P('wide', None, 'narrow'), may hold values from -6 to 6
- out_weight: bfloat16 [1024, 128], replicated, may hold values from -1 to 1
- out_bias: float32 [128], replicated, may hold values from -3 to 3
- cotangent: bfloat16 [256, 256, 128], P('wide', 'narrow'), may hold values from -0.5 to 0.5
Outputs:
- pair_update: bfloat16 [256, 256, 128], P('wide', 'narrow')
- grad_left: float32 [32, 32, 256], P('narrow', None, 'wide')
- grad_right: float32 [32, 32, 256], P('wide', None, 'narrow')
The draws below stay inside these ranges and needn't reach their ends.
All inputs are finite; a program needn't handle non-finite values.
Results may differ from the reference program's by a relative error of at most 0.0045.
Values may be sent and summed in bfloat16 or wider, within the bound.
No kernel may reach another device: no remote copies, remote signals or barrier semaphores. Data moves between devices by JAX's collectives and lax.ppermute only.
A program may use at most 64 MiB of HBM per device.

```python
import math
import jax
import jax.numpy as jnp
from jax import lax

C = 32
K = 128
S = 32
R = 256


def level_of(own_key, dims, split, low, high):
    loudness = 1.0
    for position, shards_of in split:
        draws = jax.random.uniform(jax.random.fold_in(jax.random.fold_in(own_key, 6), position), (shards_of,), jnp.float32, low / len(split), high / len(split))
        loudness = loudness * jnp.repeat(jnp.exp(draws), dims[position] // shards_of).reshape((-1,) + (1,) * (len(dims) - 1 - position))
    return loudness


def scatter_about(own_key, extent, deviation, most, split=(), held_as=jnp.bfloat16):
    factor_of = level_of(own_key, extent, split, -0.22, 0.18) if split else 1.0
    entries = jax.random.normal(own_key, extent, jnp.float32) * deviation * factor_of
    return jnp.minimum(jnp.maximum(entries, -most), most).astype(held_as)


def setup_inputs(seed: int = 0) -> dict:
    streams_of = jax.random.split(jax.random.key(seed), 6)
    left = scatter_about(streams_of[0], (S, C, R), 1.0, 6.0, ((0, 4), (2, 8)))
    right = scatter_about(streams_of[1], (S, C, R), 1.0, 6.0, ((0, 8), (2, 4)))
    out_weight = scatter_about(streams_of[2], (C * C, K), (C * C // S) ** -0.5, 1.0)
    out_bias = scatter_about(streams_of[3], (K,), 0.5, 3.0, (), jnp.float32)
    cotangent = scatter_about(streams_of[4], (R, R, K), 0.0625, 0.5, ((0, 8), (1, 4)))
    return {"left": left, "right": right, "out_weight": out_weight, "out_bias": out_bias, "cotangent": cotangent}


def reference(left, right, out_weight, out_bias, cotangent):
    residues = left.shape[2]
    rows_per_block = math.gcd(16, residues)
    total_block_count = residues // rows_per_block
    left_wide = left.astype(jnp.float32)
    right_wide = right.astype(jnp.float32)
    bias_wide = out_bias.astype(jnp.float32)

    def block_step(running, block_index):
        start = (block_index * rows_per_block).astype(jnp.int32)
        left_block = lax.dynamic_slice_in_dim(left_wide, start, rows_per_block, 2)
        outer_sum = jnp.einsum("sci,sej->ijce", left_block, right_wide) / S
        outer_flat = outer_sum.astype(jnp.bfloat16).reshape(rows_per_block * residues, C * C)
        pair_out = jnp.dot(outer_flat, out_weight, preferred_element_type=jnp.float32) + bias_wide
        pair_out = pair_out.astype(jnp.bfloat16).reshape(rows_per_block, residues, K)
        cot_block = lax.dynamic_slice_in_dim(cotangent, start, rows_per_block, 0).reshape(rows_per_block * residues, K)
        d_outer = lax.dot_general(cot_block, out_weight, (((1,), (1,)), ((), ())), preferred_element_type=jnp.float32)
        d_outer = d_outer.astype(jnp.bfloat16).reshape(rows_per_block, residues, C, C).astype(jnp.float32)
        grad_block = jnp.einsum("ijce,sej->sci", d_outer, right_wide) / S
        running = running + jnp.einsum("ijce,sci->sej", d_outer, left_block) / S
        return running, (pair_out, grad_block)

    starting_value = jnp.zeros((S, C, residues), jnp.float32)
    grad_right, (pairs, grad_blocks) = lax.scan(block_step, starting_value, jnp.arange(total_block_count, dtype=jnp.int32))
    pair_update = pairs.reshape(residues, residues, K)
    grad_left = jnp.transpose(grad_blocks, (1, 2, 0, 3)).reshape(S, C, residues)
    return pair_update, grad_left, grad_right
```

```python
import functools
import math

import jax
import jax.numpy as jnp
from jax import lax
from jax.experimental import pallas as pl
from jax.experimental.pallas import tpu as pltpu
from jax.sharding import PartitionSpec as P

LANES = 128
MXU = 256
NT = (((1,), (1,)), ((), ()))
NN = (((1,), (0,)), ((), ()))


def dot(a, b, dims):
    return lax.dot_general(a, b, dims, preferred_element_type=jnp.float32)


def block_diagonal(right_f32, channel, rows, channels, copies):
    width = right_f32.shape[1]
    one = right_f32[pl.ds(channel, rows, stride=channels), :]
    wide = jnp.concatenate([one] * copies, axis=1)
    lane = lax.broadcasted_iota(jnp.int32, wide.shape, 1)
    parts = [
        jnp.where((lane >= n * width) & (lane < (n + 1) * width), wide, 0.0) for n in range(copies)
    ]
    return jnp.concatenate(parts, axis=0).astype(jnp.bfloat16)


def place_right(place, right_refs, right_f32):
    for m, ref in enumerate(right_refs):
        rows = ref.shape[0] * ref.shape[1]
        start = pl.multiple_of((place ^ m) * rows, rows)
        block = ref[...].astype(jnp.float32).reshape(rows, ref.shape[2])
        right_f32[pl.ds(start, rows), :] = block


def place_left(place, left_refs, left_f32):
    for m, ref in enumerate(left_refs):
        for n in range(ref.shape[0]):
            left_f32[n, place ^ m] = ref[n].astype(jnp.float32)
    copies, places, part, lanes = left_f32.shape
    return left_f32[...].reshape(copies * places * part, lanes)


def place_weight(weight_ref, weight_f32, channels, weight_by_e):
    weight_f32[...] = weight_ref[...].astype(jnp.float32)
    for e in range(channels):
        rows = weight_f32[pl.ds(e, channels, stride=channels), :]
        weight_by_e[e * channels : (e + 1) * channels, :] = rows.astype(jnp.bfloat16)


def gradient_kernel(sizes, place_ref, cot_ref, weight_ref, *refs):
    n_narrow, n_wide, rows, channels, copies, groups = sizes
    left_refs, refs = refs[:n_narrow], refs[n_narrow:]
    right_refs, refs = refs[:n_wide], refs[n_wide:]
    left_outs, refs = refs[:n_narrow], refs[n_narrow:]
    right_outs, refs = refs[:n_wide], refs[n_wide:]
    left_f32, right_f32, weight_f32, weight_by_e, d_t, left_sum, right_sum = refs
    wide_place, narrow_place = place_ref[0], place_ref[1]
    columns = cot_ref.shape[1]
    group_rows = groups * channels
    place_weight(weight_ref, weight_f32, channels, weight_by_e)
    place_right(wide_place, right_refs, right_f32)
    left_mat = place_left(narrow_place, left_refs, left_f32).astype(jnp.bfloat16)

    per_dot = min(channels, MXU // channels)

    def d_group(g, _):
        slab = [cot_ref[n * groups + g] for n in range(copies)]
        slab = jnp.concatenate(slab, axis=0)
        for first in range(0, channels, per_dot):
            weight = weight_by_e[first * channels : (first + per_dot) * channels, :]
            piece = dot(weight, slab, NT).astype(jnp.bfloat16)
            for e in range(per_dot):
                start = pl.multiple_of(g * channels, channels)
                d_t[first + e, pl.ds(start, channels), :] = piece[e * channels : (e + 1) * channels]
        return 0

    lax.fori_loop(0, groups, d_group, 0, unroll=min(groups, 8))

    pack = LANES // columns
    scale = 1.0 / rows
    half = channels // pack
    low = lax.broadcasted_iota(jnp.int32, (rows, LANES), 1) < columns
    left_sum[...] = jnp.zeros_like(left_sum)

    def diagonal(outer):
        found = []
        for h in range(pack):
            total = None
            for t in range(copies // pack):
                n = t * pack + h
                piece = outer[n * rows : (n + 1) * rows, t * LANES : (t + 1) * LANES]
                total = piece if total is None else total + piece
            found.append(total)
        return found

    def e_step(first, _):
        found = []
        total = None
        for h in range(pack):
            e = first + h * half
            d_e = d_t[e]
            diag = block_diagonal(right_f32, e, rows, channels, copies)
            term = dot(d_e, diag, NT)
            total = term if total is None else total + term
            found.append(diagonal(dot(left_mat, d_e, NN)))
        left_sum[...] += total
        if pack == 1:
            result = found[0][0]
        else:
            straight = jnp.where(low, found[0][0], found[1][1])
            crossed = jnp.where(low, found[1][0], found[0][1])
            result = straight + pltpu.roll(crossed, columns, 1)
        right_sum[pl.ds(first, rows, stride=half), :] = result * scale
        return 0

    lax.fori_loop(0, half, e_step, 0, unroll=4)

    for m, ref in enumerate(right_outs):
        count = ref.shape[0]
        start = pl.multiple_of((wide_place ^ m) * count, count)
        ref[...] = right_sum[pl.ds(start, count), :].astype(ref.dtype)
    left_f32[...] = (left_sum[...].T * scale).reshape(left_f32.shape)
    for m, ref in enumerate(left_outs):
        for n in range(copies):
            ref[n] = left_f32[n, narrow_place ^ m].astype(ref.dtype)


def forward_kernel(sizes, place_ref, weight_ref, bias_ref, *refs):
    n_narrow, n_wide, rows, channels, copies, groups = sizes
    left_refs, refs = refs[:n_narrow], refs[n_narrow:]
    right_refs, refs = refs[:n_wide], refs[n_wide:]
    out_ref, left_f32, right_f32, weight_f32, weight_by_e, outer_t = refs
    wide_place, narrow_place = place_ref[0], place_ref[1]
    columns = out_ref.shape[1]
    place_weight(weight_ref, weight_f32, channels, weight_by_e)
    place_right(wide_place, right_refs, right_f32)
    left_t = place_left(narrow_place, left_refs, left_f32).T.astype(jnp.bfloat16)
    scale = 1.0 / rows
    bias = bias_ref[...]
    weight_t = weight_by_e[...].astype(jnp.float32).T.astype(jnp.bfloat16)

    def e_step(e, _):
        diag = block_diagonal(right_f32, e, rows, channels, copies)
        outer = (dot(left_t, diag, NN) * scale).astype(jnp.bfloat16)
        start = pl.multiple_of(e * channels, channels)
        for g in range(groups):
            outer_t[g, pl.ds(start, channels), :] = outer[g * channels : (g + 1) * channels]
        return 0

    lax.fori_loop(0, channels, e_step, 0, unroll=4)

    def g_step(g, _):
        pair = dot(weight_t, outer_t[g], NN).T + bias
        pair = pair.astype(jnp.bfloat16)
        for n in range(copies):
            out_ref[n * groups + g] = pair[n * columns : (n + 1) * columns]
        return 0

    lax.fori_loop(0, groups, g_step, 0, unroll=min(groups, 4))


def sum_kernel(n_narrow, n_wide, *refs):
    left_refs, refs = refs[:n_narrow], refs[n_narrow:]
    right_refs, (left_out, right_out) = refs[:n_wide], refs[n_wide:]
    total = left_refs[0][...]
    for ref in left_refs[1:]:
        total = total + ref[...].astype(jnp.float32)
    left_out[...] = total
    total = right_refs[0][...]
    for ref in right_refs[1:]:
        total = total + ref[...].astype(jnp.float32)
    rows, channels, columns = right_out.shape
    pack = LANES // columns
    half = channels // pack
    for s in range(rows):
        part = total[s * half : (s + 1) * half]
        for h in range(pack):
            right_out[s, h * half : (h + 1) * half, :] = part[:, h * columns : (h + 1) * columns]


def exchange(x, axis, m):
    size = lax.axis_size(axis)
    return lax.ppermute(x, axis, [(n, n ^ m) for n in range(size)])


def vmem(count):
    return [pl.BlockSpec(memory_space=pltpu.VMEM)] * count


def local(left, right, out_weight, out_bias, cotangent):
    n_narrow, n_wide = lax.axis_size("narrow"), lax.axis_size("wide")
    part, channels, tile_rows = left.shape
    right_part, _, columns = right.shape
    width = cotangent.shape[2]
    rows = part * n_narrow
    copies = MXU // columns
    groups = tile_rows // copies
    pack = LANES // columns
    sizes = (n_narrow, n_wide, rows, channels, copies, groups)
    place = jnp.stack([lax.axis_index("wide"), lax.axis_index("narrow")]).astype(jnp.int32)

    lefts = left.reshape(part, channels, copies, groups).transpose(2, 0, 3, 1)
    lefts = lefts.reshape(copies, part, groups * channels)
    lefts = [lefts] + [exchange(lefts, "narrow", m) for m in range(1, n_narrow)]
    rights = [right] + [exchange(right, "wide", m) for m in range(1, n_wide)]

    def left_type(m):
        kind = jnp.bfloat16 if m else jnp.float32
        return jax.ShapeDtypeStruct((copies, part, groups * channels), kind)

    def right_type(m):
        kind = jnp.bfloat16 if m else jnp.float32
        return jax.ShapeDtypeStruct((right_part * channels // pack, LANES), kind)

    f32, bf16 = jnp.float32, jnp.bfloat16
    shared = [
        pltpu.VMEM((copies, n_narrow, part, groups * channels), f32),
        pltpu.VMEM((rows * channels, columns), f32),
        pltpu.VMEM((channels * channels, width), f32),
        pltpu.VMEM((channels * channels, width), bf16),
    ]
    smem = pl.BlockSpec(memory_space=pltpu.SMEM)
    partials = pl.pallas_call(
        functools.partial(gradient_kernel, sizes),
        in_specs=[smem] + vmem(2 + n_narrow + n_wide),
        out_specs=vmem(n_narrow + n_wide),
        out_shape=[left_type(m) for m in range(n_narrow)] + [right_type(m) for m in range(n_wide)],
        scratch_shapes=shared
        + [
            pltpu.VMEM((channels, groups * channels, copies * columns), bf16),
            pltpu.VMEM((groups * channels, copies * rows), f32),
            pltpu.VMEM((rows * channels // pack, LANES), f32),
        ],
        name="gradients",
    )(place, cotangent, out_weight, *lefts, *rights)
    left_parts, right_parts = partials[:n_narrow], partials[n_narrow:]
    left_parts = [left_parts[0]] + [exchange(left_parts[m], "narrow", m) for m in range(1, n_narrow)]
    right_parts = [right_parts[0]] + [exchange(right_parts[m], "wide", m) for m in range(1, n_wide)]

    pair_update = pl.pallas_call(
        functools.partial(forward_kernel, sizes),
        in_specs=[smem] + vmem(2 + n_narrow + n_wide),
        out_specs=vmem(1)[0],
        out_shape=jax.ShapeDtypeStruct(cotangent.shape, bf16),
        scratch_shapes=shared
        + [pltpu.VMEM((groups, channels * channels, copies * columns), bf16)],
        name="forward",
        cost_estimate=pl.CostEstimate(flops=2 * 10**9, bytes_accessed=2**20, transcendentals=0),
    )(place, out_weight, out_bias.reshape(1, width), *lefts, *rights)

    grad_left, grad_right = pl.pallas_call(
        functools.partial(sum_kernel, n_narrow, n_wide),
        in_specs=vmem(n_narrow + n_wide),
        out_specs=vmem(2),
        out_shape=[left_type(0), jax.ShapeDtypeStruct((right_part, channels, columns), f32)],
        name="sums",
    )(*left_parts, *right_parts)
    grad_left = grad_left.reshape(copies, part, groups, channels).transpose(1, 3, 0, 2)
    return pair_update, grad_left.reshape(part, channels, tile_rows), grad_right


def solution(mesh):
    return jax.shard_map(
        local,
        mesh=mesh,
        in_specs=(
            P("narrow", None, "wide"),
            P("wide", None, "narrow"),
            P(),
            P(),
            P("wide", "narrow", None),
        ),
        out_specs=(P("wide", "narrow", None), P("narrow", None, "wide"), P("wide", None, "narrow")),
        check_vma=False,
    )
```

```python
import functools

import jax
import jax.numpy as jnp
from jax import lax
from jax.experimental import pallas as pl
from jax.experimental.pallas import tpu as pltpu
from jax.sharding import PartitionSpec as P


LANES = 128
MXU = 256
NT = (((1,), (1,)), ((), ()))
NN = (((1,), (0,)), ((), ()))


def dot(a, b, dims):
    return lax.dot_general(a, b, dims, preferred_element_type=jnp.float32)


def loop(count, body, small):
    if small:
        for n in range(count):
            body(n)
    else:
        lax.fori_loop(0, count, lambda n, c: (body(n), c)[1], 0)


def block_transpose(tile):
    size, lanes = tile.shape
    width = lanes // size
    row = lax.broadcasted_iota(jnp.int32, tile.shape, 0)
    block = lax.broadcasted_iota(jnp.int32, tile.shape, 1) // width
    result = tile
    for d in range(1, size):
        moved = pltpu.roll(pltpu.roll(tile, size - d, 0), width * d, 1)
        result = jnp.where(block == (row + d) % size, moved, result)
    return result


def block_diagonal(right_f32, first, rows, channels, columns, copies):
    pack = LANES // columns
    here = right_f32[pl.ds(first, rows, stride=channels // pack), :]
    lane = lax.broadcasted_iota(jnp.int32, here.shape, 1) // columns
    zero = jnp.zeros_like(here)
    moved = [here] + [pltpu.roll(here, n * columns, 1) for n in range(1, pack)]
    found = []
    for h in range(pack):
        blocks = []
        for n in range(copies):
            part = jnp.where(lane == n % pack, moved[(n - h) % pack], zero)
            tiles = [part if t == n // pack else zero for t in range(copies // pack)]
            blocks.append(jnp.concatenate(tiles, axis=1))
        found.append(jnp.concatenate(blocks, axis=0).astype(jnp.bfloat16))
    return found


def place_right(right_refs, right_f32):
    place = lax.axis_index("wide")
    for ref, keys in right_refs:
        rows = ref.shape[1]
        for n, key in enumerate(keys):
            start = pl.multiple_of((place ^ key) * rows, rows)
            right_f32[pl.ds(start, rows), :] = ref[n].astype(jnp.float32)


def place_left(left_refs, left_f32):
    place = lax.axis_index("narrow")
    for ref, keys in left_refs:
        for n, key in enumerate(keys):
            for copy in range(ref.shape[1]):
                left_f32[copy, place ^ key] = ref[n, copy].astype(jnp.float32)
    copies, places, part, lanes = left_f32.shape
    return left_f32[...].reshape(copies * places * part, lanes)


def dense(ref, out):
    rows, channels, columns = ref.shape
    pack = LANES // columns
    half = channels // pack
    for s in range(rows):
        block = ref[s].astype(jnp.float32)
        block = [block[h * half : (h + 1) * half] for h in range(pack)]
        out[s * half : (s + 1) * half, :] = jnp.concatenate(block, axis=1).astype(out.dtype)


def prepare_kernel(inside, *refs):
    sources, (left_out, *outs), (left_ref, sent) = refs[:4], refs[4:8], refs[8:]
    moves = [
        pltpu.make_async_copy(source, target, sent.at[n])
        for n, (source, target) in enumerate(zip(sources, [left_ref] + outs))
    ]
    for move in moves:
        move.start()
    moves[0].wait()
    if inside:
        part, channels, tile_rows = left_ref.shape
        flat = left_ref[...].astype(jnp.float32).reshape(part * channels, tile_rows).T
        for n in range(left_out.shape[1]):
            piece = block_transpose(flat[n * part : (n + 1) * part])
            left_out[0, n] = piece.astype(left_out.dtype)
    else:
        left_out[0] = left_ref[...]
    for move in moves[1:]:
        move.wait()


def weight_kernel(weight_ref, by_e_ref, transposed_ref, weight_f32):
    channels = by_e_ref.shape[0]
    weight_f32[...] = weight_ref[...].astype(jnp.float32)
    for e in range(channels):
        by_e_ref[e] = weight_f32[pl.ds(e, channels, stride=channels), :].astype(jnp.bfloat16)
    flat = by_e_ref[...].reshape(channels * channels, weight_ref.shape[1])
    transposed_ref[...] = flat.astype(jnp.float32).T.astype(jnp.bfloat16)


def stack_kernel(raw, one, other, *refs):
    out = refs[-1]
    count = out.shape[0] // 2
    if raw:
        dense(one, out.at[0])
        dense(other, out.at[1])
    else:
        out[:count] = one[...]
        out[count:] = other[...]


def d_outer_kernel(sizes, first, cot_ref, weight_ref, d_ref):
    _, channels, copies, groups, _ = sizes
    count = d_ref.shape[1] // channels
    per_dot = min(channels, MXU // channels)

    def step(g):
        slab = [cot_ref[n * groups + first + g] for n in range(copies)]
        slab = jnp.concatenate(slab, axis=0)
        for start in range(0, channels, per_dot):
            weight = weight_ref[start : start + per_dot].reshape(per_dot * channels, -1)
            piece = dot(weight, slab, NT).astype(jnp.bfloat16)
            for e in range(per_dot):
                at = pl.ds(g * channels, channels)
                d_ref[start + e, at, :] = piece[e * channels : (e + 1) * channels]

    loop(count, step, count <= 8)


def gradient_kernel(sizes, left_keys, right_keys, *refs):
    rows, channels, copies, _, columns = sizes
    n_left, n_right = len(left_keys), len(right_keys)
    left_refs, refs = list(zip(refs[:n_left], left_keys)), refs[n_left:]
    right_refs, refs = list(zip(refs[:n_right], right_keys)), refs[n_right:]
    d_refs, refs = refs[:-8], refs[-8:]
    left_kept, left_sent, right_kept, right_sent, left_f32, right_f32, left_sum, right_sum = refs
    place_right(right_refs, right_f32)
    left_mat = place_left(left_refs, left_f32).astype(jnp.bfloat16)
    pack = LANES // columns
    scale = 1.0 / rows
    half = channels // pack
    low = lax.broadcasted_iota(jnp.int32, (rows, LANES), 1) < columns
    small = left_mat.shape[1] <= MXU

    def diagonal(outer):
        found = []
        for h in range(pack):
            total = None
            for t in range(copies // pack):
                n = t * pack + h
                piece = outer[n * rows : (n + 1) * rows, t * LANES : (t + 1) * LANES]
                total = piece if total is None else total + piece
            found.append(total)
        return found

    if not small:
        left_sum[...] = jnp.zeros_like(left_sum)
    totals = []

    def step(first):
        found = []
        diag = block_diagonal(right_f32, first, rows, channels, columns, copies)
        for h in range(pack):
            e = first + h * half
            d_e = jnp.concatenate([ref[e] for ref in d_refs], axis=0)
            term = dot(d_e, diag[h], NT)
            if small:
                totals.append(term)
            else:
                left_sum[...] += term
            found.append(diagonal(dot(left_mat, d_e, NN)))
        if pack == 1:
            result = found[0][0]
        else:
            straight = jnp.where(low, found[0][0], found[1][1])
            crossed = jnp.where(low, found[1][0], found[0][1])
            result = straight + pltpu.roll(crossed, columns, 1)
        right_sum[pl.ds(first, rows, stride=half), :] = result * scale

    loop(half, step, small)
    if small:
        total = totals[0]
        for term in totals[1:]:
            total = total + term
        left_sum[...] = total

    place = lax.axis_index("wide")
    for n in range(right_kept.shape[0]):
        count = right_kept.shape[1]
        for key, ref in ((2 * n, right_kept), (2 * n + 1, right_sent)):
            start = pl.multiple_of((place ^ key) * count, count)
            ref[n] = right_sum[pl.ds(start, count), :].astype(ref.dtype)
    left_f32[...] = (left_sum[...].T * scale).reshape(left_f32.shape)
    place = lax.axis_index("narrow")
    for n in range(left_kept.shape[0]):
        for key, ref in ((2 * n, left_kept), (2 * n + 1, left_sent)):
            for copy in range(copies):
                ref[n, copy] = left_f32[copy, place ^ key].astype(ref.dtype)


def forward_kernel(sizes, left_keys, right_keys, first, aliased, *refs):
    rows, channels, copies, groups, columns = sizes
    n_left, n_right = len(left_keys), len(right_keys)
    weight_ref, bias_ref, refs = refs[0], refs[1], refs[2:]
    left_refs, refs = list(zip(refs[:n_left], left_keys)), refs[n_left:]
    right_refs, refs = list(zip(refs[:n_right], right_keys)), refs[n_right:]
    out_ref, left_f32, right_f32, outer_t, pairs, sent = refs[1:] if aliased else refs
    count = outer_t.shape[0]
    place_right(right_refs, right_f32)
    left_t = place_left(left_refs, left_f32).T.astype(jnp.bfloat16)
    left_t = left_t[first * channels : (first + count) * channels]
    pack = LANES // columns
    half = channels // pack
    scale = 1.0 / rows
    bias = bias_ref[...]
    small = count <= 8

    def e_step(start):
        diag = block_diagonal(right_f32, start, rows, channels, columns, copies)
        for h in range(pack):
            outer = (dot(left_t, diag[h], NN) * scale).astype(jnp.bfloat16)
            at = pl.ds((start + h * half) * channels, channels)
            for g in range(count):
                outer_t[g, at, :] = outer[g * channels : (g + 1) * channels]

    loop(half, e_step, small)

    def g_step(g):
        pair = dot(weight_ref[...], outer_t[g], NN).T + bias
        pair = pair.astype(jnp.bfloat16)
        for n in range(copies):
            pairs[n * count + g] = pair[n * columns : (n + 1) * columns]

    loop(count, g_step, small)
    moves = []
    for n in range(copies):
        source = pairs.at[pl.ds(n * count, count)]
        target = out_ref.at[pl.ds(n * groups + first, count)]
        moves.append(pltpu.make_async_copy(source, target, sent.at[n]))
        moves[-1].start()
    for move in moves:
        move.wait()


def add_kernel(*refs):
    (left_kept, left_new, right_kept, right_new), outs = refs[:4], refs[4:]
    for n in range(left_kept.shape[0]):
        total = left_kept[n] + left_new[n].astype(jnp.float32)
        outs[n][...] = total.astype(outs[n].dtype)
    outs = outs[left_kept.shape[0] :]
    for n in range(right_kept.shape[0]):
        total = right_kept[n] + right_new[n].astype(jnp.float32)
        outs[n][...] = total.astype(outs[n].dtype)


def sum_kernel(n_left, inside, *refs):
    left_refs, refs = refs[:n_left], refs[n_left:]
    right_refs, (left_out, right_out) = refs[:-2], refs[-2:]
    total = left_refs[0][...]
    for ref in left_refs[1:]:
        total = total + ref[...].astype(jnp.float32)
    if inside:
        total = jnp.concatenate([block_transpose(total[n]) for n in range(total.shape[0])], axis=0)
        left_out[...] = total.T.reshape(left_out.shape)
    else:
        left_out[...] = total
    total = right_refs[0][...]
    for ref in right_refs[1:]:
        total = total + ref[...].astype(jnp.float32)
    rows, channels, columns = right_out.shape
    pack = LANES // columns
    half = channels // pack
    for s in range(rows):
        part = total[s * half : (s + 1) * half]
        for h in range(pack):
            right_out[s, h * half : (h + 1) * half, :] = part[:, h * columns : (h + 1) * columns]


def exchange(x, axis, m):
    size = lax.axis_size(axis)
    return lax.ppermute(x, axis, [(n, n ^ m) for n in range(size)])


def powers(size):
    return [1 << n for n in range(size.bit_length() - 1)]


def vmem(count):
    return [pl.BlockSpec(memory_space=pltpu.VMEM)] * count


def tile(left, right, out_weight, out_bias, cotangent):
    n_narrow, n_wide = lax.axis_size("narrow"), lax.axis_size("wide")
    part, channels, tile_rows = left.shape
    right_part, _, columns = right.shape
    width = cotangent.shape[2]
    rows = part * n_narrow
    copies = MXU // columns
    groups = tile_rows // copies
    pack = LANES // columns
    inside = part == groups and channels * part == MXU
    halves = 2
    count = groups // halves
    sizes = (rows, channels, copies, groups, columns)
    f32, bf16 = jnp.float32, jnp.bfloat16
    shape = jax.ShapeDtypeStruct
    work = channels * channels * tile_rows * columns
    limit = min(56 << 20, max(12 << 20, 3 * work))
    flops = 2 * work * width
    anywhere = pl.BlockSpec(memory_space=pl.ANY)
    outside = pl.BlockSpec(memory_space=pltpu.HBM)

    def call(kernel, outs, args, scratch=(), cost=0, in_specs=None, out_specs=None, **more):
        return pl.pallas_call(
            kernel,
            in_specs=in_specs or vmem(len(args)),
            out_specs=out_specs or vmem(len(outs)),
            out_shape=outs,
            scratch_shapes=scratch,
            compiler_params=pltpu.CompilerParams(vmem_limit_bytes=limit),
            cost_estimate=pl.CostEstimate(flops=cost, bytes_accessed=1 << 16, transcendentals=0),
            **more,
        )(*args)

    left_shape = (copies, part, groups * channels)
    right_shape = (right_part * channels // pack, LANES)

    hbm = functools.partial(pltpu.with_memory_space_constraint, memory_space=pltpu.HBM)

    steps = powers(n_wide)[1:] + [1]
    right_new = exchange(right, "wide", steps[0])
    source = left
    if not inside:
        source = left.reshape(part, channels, copies, groups).transpose(2, 0, 3, 1)
        source = source.reshape(left_shape)
    sources = [source, right, out_weight, cotangent]
    lefts, rights, weight, cot = call(
        functools.partial(prepare_kernel, inside),
        [shape((1,) + left_shape, bf16)] + [shape(v.shape, bf16) for v in sources[1:]],
        [hbm(v) for v in sources],
        [pltpu.VMEM(source.shape, bf16), pltpu.SemaphoreType.DMA((4,))],
        cost=flops // 16,
        in_specs=[outside] * 4,
    )
    by_e, transposed = call(
        weight_kernel,
        [shape((channels, channels, width), bf16), shape((width, channels * channels), bf16)],
        [weight],
        [pltpu.VMEM(weight.shape, f32)],
        cost=flops // 8,
    )

    def stack(one, other, raw, after=()):
        shapes = right_shape if raw else one.shape[1:]
        outs = [shape((2 if raw else 2 * one.shape[0],) + shapes, bf16)]
        args = [one, other, *after]
        specs = vmem(2) + [anywhere] * len(after)
        return call(functools.partial(stack_kernel, raw), outs, args, in_specs=specs)[0]

    d_shape = shape((channels, count * channels, copies * columns), bf16)
    d_outer = []
    for n in range(halves):
        kernel = functools.partial(d_outer_kernel, sizes, n * count)
        d_outer += call(kernel, [d_shape], [cot, by_e], cost=flops // halves)

    keys = [0]
    for n, m in enumerate(steps):
        if n:
            right_new = exchange(rights, "wide", m)
        new = [k ^ m for k in keys]
        if n + 1 < len(steps):
            rights = stack(rights, right_new, n == 0, d_outer[n : n + 1])
            keys = keys + new
    right_keys, rights = (keys, new), [rights, right_new]

    keys = [0]
    steps = powers(n_narrow)[::-1]
    for n, m in enumerate(steps):
        left_new = exchange(lefts, "narrow", m)
        new = [k ^ m for k in keys]
        if n + 1 < len(steps):
            lefts = stack(lefts, left_new, False, d_outer[1:2] if n == 0 else ())
            keys = keys + new
    left_keys, lefts = (keys, new), [lefts, left_new]

    left_f32 = pltpu.VMEM((copies, n_narrow, part, groups * channels), f32)
    right_f32 = pltpu.VMEM((rows * channels // pack, LANES), f32)
    far, near = n_narrow // 2, n_wide // 2
    left_kept, left_sent, right_kept, right_sent = call(
        functools.partial(gradient_kernel, sizes, left_keys, right_keys),
        [
            shape((far,) + left_shape, f32),
            shape((far,) + left_shape, bf16),
            shape((near,) + right_shape, f32),
            shape((near,) + right_shape, bf16),
        ],
        [*lefts, *rights, *d_outer],
        [
            left_f32,
            right_f32,
            pltpu.VMEM((groups * channels, copies * rows), f32),
            pltpu.VMEM((rows * channels // pack, LANES), f32),
        ],
        cost=flops * 2,
    )
    left_new = exchange(left_sent, "narrow", 1)
    right_new = exchange(right_sent, "wide", 1)

    def forward(first, before):
        args = [transposed, out_bias.reshape(1, width), *lefts, *rights]
        specs, more = vmem(len(args)), {}
        if before is not None:
            more = {"input_output_aliases": {len(args): 0}}
            args, specs = args + [before], specs + [anywhere]
        return call(
            functools.partial(
                forward_kernel, sizes, left_keys, right_keys, first, before is not None
            ),
            [shape(cotangent.shape, bf16)],
            args,
            [
                left_f32,
                right_f32,
                pltpu.VMEM((count, channels * channels, copies * columns), bf16),
                pltpu.VMEM((copies * count, columns, width), bf16),
                pltpu.SemaphoreType.DMA((copies,)),
            ],
            cost=flops,
            in_specs=specs,
            out_specs=[anywhere],
            **more,
        )[0]

    pair_update = forward(0, None)
    sums = call(
        add_kernel,
        [shape(left_shape, bf16 if n else f32) for n in range(far)]
        + [shape(right_shape, bf16 if n else f32) for n in range(near)],
        [left_kept, left_new, right_kept, right_new],
    )
    left_sums = [exchange(v, "narrow", 2 * n) if n else v for n, v in enumerate(sums[:far])]
    right_sums = [exchange(v, "wide", 2 * n) if n else v for n, v in enumerate(sums[far:])]
    for n in range(1, halves):
        pair_update = forward(n * count, pair_update)

    grad_left, grad_right = call(
        functools.partial(sum_kernel, far, inside),
        [
            shape((part, channels, tile_rows) if inside else left_shape, f32),
            shape((right_part, channels, columns), f32),
        ],
        [*left_sums, *right_sums],
    )
    if not inside:
        grad_left = grad_left.reshape(copies, part, groups, channels).transpose(1, 3, 0, 2)
        grad_left = grad_left.reshape(part, channels, tile_rows)
    return pair_update, grad_left, grad_right


def solution(mesh):
    return jax.shard_map(
        tile,
        mesh=mesh,
        in_specs=(
            P("narrow", None, "wide"),
            P("wide", None, "narrow"),
            P(),
            P(),
            P("wide", "narrow", None),
        ),
        out_specs=(P("wide", "narrow", None), P("narrow", None, "wide"), P("wide", None, "narrow")),
        check_vma=False,
    )
```

```python
import functools

import jax
import jax.numpy as jnp
from jax import lax
from jax.experimental import pallas as pl
from jax.experimental.pallas import tpu as pltpu
from jax.sharding import PartitionSpec as P


LANES = 128
MXU = 256
NT = (((1,), (1,)), ((), ()))
NN = (((1,), (0,)), ((), ()))


def dot(a, b, dims):
    return lax.dot_general(a, b, dims, preferred_element_type=jnp.float32)


def loop(count, body, small):
    if small:
        for n in range(count):
            body(n)
    else:
        lax.fori_loop(0, count, lambda n, c: (body(n), c)[1], 0)


def block_transpose(tile):
    size, lanes = tile.shape
    width = lanes // size
    row = lax.broadcasted_iota(jnp.int32, tile.shape, 0)
    block = lax.broadcasted_iota(jnp.int32, tile.shape, 1) // width
    result = tile
    for d in range(1, size):
        moved = pltpu.roll(pltpu.roll(tile, size - d, 0), width * d, 1)
        result = jnp.where(block == (row + d) % size, moved, result)
    return result


def block_diagonal(right_f32, first, rows, channels, columns, copies):
    pack = LANES // columns
    here = right_f32[pl.ds(first, rows, stride=channels // pack), :]
    lane = lax.broadcasted_iota(jnp.int32, here.shape, 1) // columns
    zero = jnp.zeros_like(here)
    moved = [here] + [pltpu.roll(here, n * columns, 1) for n in range(1, pack)]
    found = []
    for h in range(pack):
        blocks = []
        for n in range(copies):
            part = jnp.where(lane == n % pack, moved[(n - h) % pack], zero)
            tiles = [part if t == n // pack else zero for t in range(copies // pack)]
            blocks.append(jnp.concatenate(tiles, axis=1))
        found.append(jnp.concatenate(blocks, axis=0).astype(jnp.bfloat16))
    return found


def place_right(right_refs, right_f32):
    place = lax.axis_index("wide")
    for ref, keys in right_refs:
        rows = ref.shape[1]
        for n, key in enumerate(keys):
            start = pl.multiple_of((place ^ key) * rows, rows)
            right_f32[pl.ds(start, rows), :] = ref[n].astype(jnp.float32)


def place_left(left_refs, left_f32):
    place = lax.axis_index("narrow")
    for ref, keys in left_refs:
        for n, key in enumerate(keys):
            for copy in range(ref.shape[1]):
                left_f32[copy, place ^ key] = ref[n, copy].astype(jnp.float32)
    copies, places, part, lanes = left_f32.shape
    return left_f32[...].reshape(copies * places * part, lanes)


def dense(ref, out):
    rows, channels, columns = ref.shape
    pack = LANES // columns
    half = channels // pack
    for s in range(rows):
        block = ref[s].astype(jnp.float32)
        block = [block[h * half : (h + 1) * half] for h in range(pack)]
        out[s * half : (s + 1) * half, :] = jnp.concatenate(block, axis=1).astype(out.dtype)


def left_layout(ref, out):
    part, channels, tile_rows = ref.shape
    flat = ref[...].astype(jnp.float32).reshape(part * channels, tile_rows).T
    for n in range(out.shape[0]):
        out[n] = block_transpose(flat[n * part : (n + 1) * part]).astype(out.dtype)


def prepare_kernel(inside, *refs):
    sources, (left_out, *outs), (left_ref, sent) = refs[:4], refs[4:8], refs[8:]
    moves = [
        pltpu.make_async_copy(source, target, sent.at[n])
        for n, (source, target) in enumerate(zip(sources, [left_ref] + outs))
    ]
    for move in moves:
        move.start()
    moves[0].wait()
    if inside:
        left_layout(left_ref, left_out.at[0])
    else:
        left_out[0] = left_ref[...]
    for move in moves[1:]:
        move.wait()


def weight_kernel(weight_ref, by_e_ref, transposed_ref, weight_f32):
    channels = by_e_ref.shape[0]
    weight_f32[...] = weight_ref[...].astype(jnp.float32)
    for e in range(channels):
        by_e_ref[e] = weight_f32[pl.ds(e, channels, stride=channels), :].astype(jnp.bfloat16)
    flat = by_e_ref[...].reshape(channels * channels, weight_ref.shape[1])
    transposed_ref[...] = flat.astype(jnp.float32).T.astype(jnp.bfloat16)


def stack_kernel(change, one, other, *refs):
    out = refs[-1]
    count = out.shape[0] // 2
    if change is dense:
        dense(one, out.at[0])
        dense(other, out.at[1])
    else:
        out[:count] = one[...]
        out[count:] = other[...]


def d_outer_kernel(sizes, first, cot_ref, weight_ref, d_ref):
    _, channels, copies, groups, _ = sizes
    count = d_ref.shape[1] // channels
    per_dot = min(channels, MXU // channels)

    def step(g):
        slab = [cot_ref[n * groups + first + g] for n in range(copies)]
        slab = jnp.concatenate(slab, axis=0)
        for start in range(0, channels, per_dot):
            weight = weight_ref[start : start + per_dot].reshape(per_dot * channels, -1)
            piece = dot(weight, slab, NT).astype(jnp.bfloat16)
            for e in range(per_dot):
                at = pl.ds(g * channels, channels)
                d_ref[start + e, at, :] = piece[e * channels : (e + 1) * channels]

    loop(count, step, count <= 8)


def gradient_kernel(sizes, left_keys, right_keys, *refs):
    rows, channels, copies, _, columns = sizes
    n_left, n_right = len(left_keys), len(right_keys)
    left_refs, refs = list(zip(refs[:n_left], left_keys)), refs[n_left:]
    right_refs, refs = list(zip(refs[:n_right], right_keys)), refs[n_right:]
    d_refs, refs = refs[:-8], refs[-8:]
    left_kept, left_sent, right_kept, right_sent, left_f32, right_f32, left_sum, right_sum = refs
    place_right(right_refs, right_f32)
    left_mat = place_left(left_refs, left_f32).astype(jnp.bfloat16)
    pack = LANES // columns
    scale = 1.0 / rows
    half = channels // pack
    low = lax.broadcasted_iota(jnp.int32, (rows, LANES), 1) < columns
    small = left_mat.shape[1] <= MXU

    def diagonal(outer):
        found = []
        for h in range(pack):
            total = None
            for t in range(copies // pack):
                n = t * pack + h
                piece = outer[n * rows : (n + 1) * rows, t * LANES : (t + 1) * LANES]
                total = piece if total is None else total + piece
            found.append(total)
        return found

    if not small:
        left_sum[...] = jnp.zeros_like(left_sum)
    totals = []

    def step(first):
        found = []
        diag = block_diagonal(right_f32, first, rows, channels, columns, copies)
        for h in range(pack):
            e = first + h * half
            d_e = jnp.concatenate([ref[e] for ref in d_refs], axis=0)
            term = dot(d_e, diag[h], NT)
            if small:
                totals.append(term)
            else:
                left_sum[...] += term
            found.append(diagonal(dot(left_mat, d_e, NN)))
        if pack == 1:
            result = found[0][0]
        else:
            straight = jnp.where(low, found[0][0], found[1][1])
            crossed = jnp.where(low, found[1][0], found[0][1])
            result = straight + pltpu.roll(crossed, columns, 1)
        right_sum[pl.ds(first, rows, stride=half), :] = result * scale

    loop(half, step, small)
    if small:
        total = totals[0]
        for term in totals[1:]:
            total = total + term
        left_sum[...] = total

    place = lax.axis_index("wide")
    for n in range(right_kept.shape[0]):
        count = right_kept.shape[1]
        for key, ref in ((2 * n, right_kept), (2 * n + 1, right_sent)):
            start = pl.multiple_of((place ^ key) * count, count)
            ref[n] = right_sum[pl.ds(start, count), :].astype(ref.dtype)
    left_f32[...] = (left_sum[...].T * scale).reshape(left_f32.shape)
    place = lax.axis_index("narrow")
    for n in range(left_kept.shape[0]):
        for key, ref in ((2 * n, left_kept), (2 * n + 1, left_sent)):
            for copy in range(copies):
                ref[n, copy] = left_f32[copy, place ^ key].astype(ref.dtype)


def forward_kernel(sizes, left_keys, right_keys, *refs):
    rows, channels, copies, groups, columns = sizes
    n_left, n_right = len(left_keys), len(right_keys)
    weight_ref, bias_ref, refs = refs[0], refs[1], refs[2:]
    left_refs, refs = list(zip(refs[:n_left], left_keys)), refs[n_left:]
    right_refs, refs = list(zip(refs[:n_right], right_keys)), refs[n_right:]
    out_ref, left_f32, right_f32, outer_t = refs
    place_right(right_refs, right_f32)
    left_t = place_left(left_refs, left_f32).T.astype(jnp.bfloat16)
    pack = LANES // columns
    half = channels // pack
    scale = 1.0 / rows
    bias = bias_ref[...]
    small = groups <= 8

    def e_step(start):
        diag = block_diagonal(right_f32, start, rows, channels, columns, copies)
        for h in range(pack):
            outer = (dot(left_t, diag[h], NN) * scale).astype(jnp.bfloat16)
            at = pl.ds((start + h * half) * channels, channels)
            for g in range(groups):
                outer_t[g, at, :] = outer[g * channels : (g + 1) * channels]

    loop(half, e_step, small)

    def g_step(g):
        pair = dot(weight_ref[...], outer_t[g], NN).T + bias
        pair = pair.astype(jnp.bfloat16)
        for n in range(copies):
            out_ref[n * groups + g] = pair[n * columns : (n + 1) * columns]

    loop(groups, g_step, small)


def add_kernel(kept, new, *outs):
    for n, out in enumerate(outs):
        out[...] = (kept[n] + new[n].astype(jnp.float32)).astype(out.dtype)


def last_kernel(n_left, n_right, inside, pairs, *refs):
    left_refs, refs = refs[:n_left], refs[n_left:]
    right_refs, refs = refs[:n_right], refs[n_right:]
    outs, (left_out, right_out, sent) = refs[:3], refs[3:]
    moves = [
        pltpu.make_async_copy(source, target, sent.at[n])
        for n, (source, target) in enumerate(zip((pairs, left_out, right_out), outs))
    ]
    moves[0].start()
    total = left_refs[0][...]
    for ref in left_refs[1:]:
        total = total + ref[...].astype(jnp.float32)
    if inside:
        total = jnp.concatenate([block_transpose(total[n]) for n in range(total.shape[0])], axis=0)
        left_out[...] = total.T.reshape(left_out.shape)
    else:
        left_out[...] = total
    moves[1].start()
    total = right_refs[0][...]
    for ref in right_refs[1:]:
        total = total + ref[...].astype(jnp.float32)
    rows, channels, columns = right_out.shape
    pack = LANES // columns
    half = channels // pack
    for s in range(rows):
        part = total[s * half : (s + 1) * half]
        for h in range(pack):
            right_out[s, h * half : (h + 1) * half, :] = part[:, h * columns : (h + 1) * columns]
    moves[2].start()
    for move in moves:
        move.wait()


def exchange(x, axis, m):
    size = lax.axis_size(axis)
    return lax.ppermute(x, axis, [(n, n ^ m) for n in range(size)])


def powers(size):
    return [1 << n for n in range(size.bit_length() - 1)]


def vmem(count):
    return [pl.BlockSpec(memory_space=pltpu.VMEM)] * count


def tile(left, right, out_weight, out_bias, cotangent):
    n_narrow, n_wide = lax.axis_size("narrow"), lax.axis_size("wide")
    part, channels, tile_rows = left.shape
    right_part, _, columns = right.shape
    width = cotangent.shape[2]
    rows = part * n_narrow
    copies = MXU // columns
    groups = tile_rows // copies
    pack = LANES // columns
    inside = part == groups and channels * part == MXU
    halves = 2
    count = groups // halves
    sizes = (rows, channels, copies, groups, columns)
    f32, bf16 = jnp.float32, jnp.bfloat16
    shape = jax.ShapeDtypeStruct
    work = channels * channels * tile_rows * columns
    limit = min(56 << 20, max(12 << 20, 3 * work))
    flops = 2 * work * width
    anywhere = pl.BlockSpec(memory_space=pl.ANY)
    outside = pl.BlockSpec(memory_space=pltpu.HBM)

    def call(kernel, outs, args, scratch=(), cost=0, in_specs=None, out_specs=None, **more):
        return pl.pallas_call(
            kernel,
            in_specs=in_specs or vmem(len(args)),
            out_specs=out_specs or vmem(len(outs)),
            out_shape=outs,
            scratch_shapes=scratch,
            compiler_params=pltpu.CompilerParams(vmem_limit_bytes=limit),
            cost_estimate=pl.CostEstimate(flops=cost, bytes_accessed=1 << 16, transcendentals=0),
            **more,
        )(*args)

    left_shape = (copies, part, groups * channels)
    right_shape = (right_part * channels // pack, LANES)

    hbm = functools.partial(pltpu.with_memory_space_constraint, memory_space=pltpu.HBM)

    steps = powers(n_wide)[1:] + [1]
    narrow_steps = powers(n_narrow)[::-1]
    right_new = exchange(right, "wide", steps[0])
    source = left
    if not inside:
        source = left.reshape(part, channels, copies, groups).transpose(2, 0, 3, 1)
        source = source.reshape(left_shape)
    sources = [source, right, out_weight, cotangent]
    lefts, rights, weight, cot = call(
        functools.partial(prepare_kernel, inside),
        [shape((1,) + left_shape, bf16)] + [shape(v.shape, bf16) for v in sources[1:]],
        [hbm(v) for v in sources],
        [pltpu.VMEM(source.shape, bf16), pltpu.SemaphoreType.DMA((4,))],
        cost=flops // 16,
        in_specs=[outside] * 4,
    )
    by_e, transposed = call(
        weight_kernel,
        [shape((channels, channels, width), bf16), shape((width, channels * channels), bf16)],
        [weight],
        [pltpu.VMEM(weight.shape, f32)],
        cost=flops // 8,
    )

    def stack(one, other, change, after=()):
        total, shapes = 2 * one.shape[0], one.shape[1:]
        if change is dense:
            total, shapes = 2, right_shape
        args = [one, other, *after]
        specs = vmem(2) + [anywhere] * len(after)
        kernel = functools.partial(stack_kernel, change)
        return call(kernel, [shape((total,) + shapes, bf16)], args, in_specs=specs)[0]

    d_shape = shape((channels, count * channels, copies * columns), bf16)
    d_outer = []
    for n in range(halves):
        kernel = functools.partial(d_outer_kernel, sizes, n * count)
        d_outer += call(kernel, [d_shape], [cot, by_e], cost=flops // halves)

    keys = [0]
    for n, m in enumerate(steps):
        if n:
            right_new = exchange(rights, "wide", m)
        new = [k ^ m for k in keys]
        if n + 1 < len(steps):
            change = dense if n == 0 else None
            rights = stack(rights, right_new, change, d_outer[n : n + 1])
            keys = keys + new
    right_keys, rights = (keys, new), [rights, right_new]

    keys = [0]
    for n, m in enumerate(narrow_steps):
        left_new = exchange(lefts, "narrow", m)
        new = [k ^ m for k in keys]
        if n + 1 < len(narrow_steps):
            lefts = stack(lefts, left_new, None)
            keys = keys + new
    left_keys, lefts = (keys, new), [lefts, left_new]

    left_f32 = pltpu.VMEM((copies, n_narrow, part, groups * channels), f32)
    right_f32 = pltpu.VMEM((rows * channels // pack, LANES), f32)
    far, near = n_narrow // 2, n_wide // 2
    left_kept, left_sent, right_kept, right_sent = call(
        functools.partial(gradient_kernel, sizes, left_keys, right_keys),
        [
            shape((far,) + left_shape, f32),
            shape((far,) + left_shape, bf16),
            shape((near,) + right_shape, f32),
            shape((near,) + right_shape, bf16),
        ],
        [*lefts, *rights, *d_outer],
        [
            left_f32,
            right_f32,
            pltpu.VMEM((groups * channels, copies * rows), f32),
            pltpu.VMEM((rows * channels // pack, LANES), f32),
        ],
        cost=flops * 2,
    )
    left_new = exchange(left_sent, "narrow", 1)
    right_new = exchange(right_sent, "wide", 1)

    def add(kept, new):
        outs = [shape(kept.shape[1:], bf16 if n else f32) for n in range(kept.shape[0])]
        return list(call(add_kernel, outs, [kept, new]))

    right_sums = add(right_kept, right_new)
    for n in range(1, near):
        right_sums[n] = exchange(right_sums[n], "wide", 2 * n)
    left_sums = add(left_kept, left_new)
    for n in range(1, far):
        left_sums[n] = exchange(left_sums[n], "narrow", 2 * n)

    (pairs,) = call(
        functools.partial(forward_kernel, sizes, left_keys, right_keys),
        [shape(cotangent.shape, bf16)],
        [transposed, out_bias.reshape(1, width), *lefts, *rights],
        [left_f32, right_f32, pltpu.VMEM((groups, channels * channels, copies * columns), bf16)],
        cost=2 * flops,
    )
    last = [
        shape(cotangent.shape, bf16),
        shape((part, channels, tile_rows) if inside else left_shape, f32),
        shape((right_part, channels, columns), f32),
    ]
    pair_update, grad_left, grad_right = call(
        functools.partial(last_kernel, far, near, inside),
        last,
        [pairs, *left_sums, *right_sums],
        [pltpu.VMEM(v.shape, f32) for v in last[1:]] + [pltpu.SemaphoreType.DMA((3,))],
        out_specs=[outside] * 3,
    )
    if not inside:
        grad_left = grad_left.reshape(copies, part, groups, channels).transpose(1, 3, 0, 2)
        grad_left = grad_left.reshape(part, channels, tile_rows)
    return pair_update, grad_left, grad_right


def solution(mesh):
    return jax.shard_map(
        tile,
        mesh=mesh,
        in_specs=(
            P("narrow", None, "wide"),
            P("wide", None, "narrow"),
            P(),
            P(),
            P("wide", "narrow", None),
        ),
        out_specs=(P("wide", "narrow", None), P("narrow", None, "wide"), P("wide", None, "narrow")),
        check_vma=False,
    )
```

```python
import functools

import jax
import jax.numpy as jnp
from jax import lax
from jax.experimental import pallas as pl
from jax.experimental.pallas import tpu as pltpu
from jax.sharding import PartitionSpec as P


LANES = 128
MXU = 256
NT = (((1,), (1,)), ((), ()))
NN = (((1,), (0,)), ((), ()))


def dot(a, b, dims):
    return lax.dot_general(a, b, dims, preferred_element_type=jnp.float32)


def loop(count, body, small):
    if small:
        for n in range(count):
            body(n)
    else:
        lax.fori_loop(0, count, lambda n, c: (body(n), c)[1], 0)


def block_transpose(tile):
    size, lanes = tile.shape
    width = lanes // size
    row = lax.broadcasted_iota(jnp.int32, tile.shape, 0)
    block = lax.broadcasted_iota(jnp.int32, tile.shape, 1) // width
    result = tile
    for d in range(1, size):
        moved = pltpu.roll(pltpu.roll(tile, size - d, 0), width * d, 1)
        result = jnp.where(block == (row + d) % size, moved, result)
    return result


def block_diagonal(right_f32, first, rows, channels, columns, copies):
    pack = LANES // columns
    here = right_f32[pl.ds(first, rows, stride=channels // pack), :]
    lane = lax.broadcasted_iota(jnp.int32, here.shape, 1) // columns
    zero = jnp.zeros_like(here)
    moved = [here] + [pltpu.roll(here, n * columns, 1) for n in range(1, pack)]
    found = []
    for h in range(pack):
        blocks = []
        for n in range(copies):
            part = jnp.where(lane == n % pack, moved[(n - h) % pack], zero)
            tiles = [part if t == n // pack else zero for t in range(copies // pack)]
            blocks.append(jnp.concatenate(tiles, axis=1))
        found.append(jnp.concatenate(blocks, axis=0).astype(jnp.bfloat16))
    return found


def place_right(right_refs, right_f32):
    place = lax.axis_index("wide")
    for ref, keys in right_refs:
        rows = ref.shape[1]
        for n, key in enumerate(keys):
            start = pl.multiple_of((place ^ key) * rows, rows)
            right_f32[pl.ds(start, rows), :] = ref[n].astype(jnp.float32)


def place_left(left_refs, left_f32):
    place = lax.axis_index("narrow")
    for ref, keys in left_refs:
        for n, key in enumerate(keys):
            for copy in range(ref.shape[1]):
                left_f32[copy, place ^ key] = ref[n, copy].astype(jnp.float32)
    copies, places, part, lanes = left_f32.shape
    return left_f32[...].reshape(copies * places * part, lanes)


def dense(ref, out):
    rows, channels, columns = ref.shape
    pack = LANES // columns
    half = channels // pack
    for s in range(rows):
        block = ref[s].astype(jnp.float32)
        block = [block[h * half : (h + 1) * half] for h in range(pack)]
        out[s * half : (s + 1) * half, :] = jnp.concatenate(block, axis=1).astype(out.dtype)


def left_layout(ref, out):
    part, channels, tile_rows = ref.shape
    flat = ref[...].astype(jnp.float32).reshape(part * channels, tile_rows).T
    for n in range(out.shape[0]):
        out[n] = block_transpose(flat[n * part : (n + 1) * part]).astype(out.dtype)


def prepare_kernel(inside, *refs):
    sources, (left_out, *outs), (left_ref, sent) = refs[:4], refs[4:8], refs[8:]
    moves = [
        pltpu.make_async_copy(source, target, sent.at[n])
        for n, (source, target) in enumerate(zip(sources, [left_ref] + outs))
    ]
    for move in moves:
        move.start()
    moves[0].wait()
    if inside:
        left_layout(left_ref, left_out.at[0])
    else:
        left_out[0] = left_ref[...]
    for move in moves[1:]:
        move.wait()


def weight_kernel(weight_ref, by_e_ref, transposed_ref, weight_f32):
    channels = by_e_ref.shape[0]
    weight_f32[...] = weight_ref[...].astype(jnp.float32)
    for e in range(channels):
        by_e_ref[e] = weight_f32[pl.ds(e, channels, stride=channels), :].astype(jnp.bfloat16)
    flat = by_e_ref[...].reshape(channels * channels, weight_ref.shape[1])
    transposed_ref[...] = flat.astype(jnp.float32).T.astype(jnp.bfloat16)


def stack_kernel(change, one, other, *refs):
    out = refs[-1]
    count = out.shape[0] // 2
    if change is dense:
        dense(one, out.at[0])
        dense(other, out.at[1])
    else:
        out[:count] = one[...]
        out[count:] = other[...]


def d_outer_kernel(sizes, first, cot_ref, weight_ref, d_ref):
    _, channels, copies, groups, _ = sizes
    count = d_ref.shape[1] // channels
    per_dot = min(channels, MXU // channels)

    def step(g):
        slab = [cot_ref[n * groups + first + g] for n in range(copies)]
        slab = jnp.concatenate(slab, axis=0)
        for start in range(0, channels, per_dot):
            weight = weight_ref[start : start + per_dot].reshape(per_dot * channels, -1)
            piece = dot(weight, slab, NT).astype(jnp.bfloat16)
            for e in range(per_dot):
                at = pl.ds(g * channels, channels)
                d_ref[start + e, at, :] = piece[e * channels : (e + 1) * channels]

    loop(count, step, count <= 8)


def split_parts(total, axis, kept_ref, sent_ref):
    place = lax.axis_index(axis)
    for n in range(kept_ref.shape[0]):
        kept_ref[n] = total(place ^ (2 * n)).astype(kept_ref.dtype)
        sent_ref[n] = total(place ^ (2 * n + 1)).astype(sent_ref.dtype)


def left_gradient_kernel(sizes, right_keys, *refs):
    rows, channels, copies, groups, columns = sizes
    n_right = len(right_keys)
    right_refs, refs = list(zip(refs[:n_right], right_keys)), refs[n_right:]
    d_refs, (kept_ref, sent_ref, left_f32, right_f32, left_sum) = refs[:-5], refs[-5:]
    place_right(right_refs, right_f32)
    pack = LANES // columns
    half = channels // pack
    small = groups * channels <= MXU
    if not small:
        left_sum[...] = jnp.zeros_like(left_sum)
    totals = []

    def step(first):
        diag = block_diagonal(right_f32, first, rows, channels, columns, copies)
        for h in range(pack):
            d_e = jnp.concatenate([ref[first + h * half] for ref in d_refs], axis=0)
            term = dot(d_e, diag[h], NT)
            if small:
                totals.append(term)
            else:
                left_sum[...] += term

    loop(half, step, small)
    if small:
        total = totals[0]
        for term in totals[1:]:
            total = total + term
    else:
        total = left_sum[...]
    left_f32[...] = (total.T * (1.0 / rows)).reshape(left_f32.shape)
    split_parts(lambda place: left_f32[:, place], "narrow", kept_ref, sent_ref)


def right_gradient_kernel(sizes, left_keys, *refs):
    rows, channels, copies, _, columns = sizes
    n_left = len(left_keys)
    left_refs, refs = list(zip(refs[:n_left], left_keys)), refs[n_left:]
    d_refs, (kept_ref, sent_ref, left_f32, right_sum) = refs[:-4], refs[-4:]
    left_mat = place_left(left_refs, left_f32).astype(jnp.bfloat16)
    pack = LANES // columns
    half = channels // pack
    low = lax.broadcasted_iota(jnp.int32, (rows, LANES), 1) < columns

    def diagonal(outer):
        found = []
        for h in range(pack):
            total = None
            for t in range(copies // pack):
                n = t * pack + h
                piece = outer[n * rows : (n + 1) * rows, t * LANES : (t + 1) * LANES]
                total = piece if total is None else total + piece
            found.append(total)
        return found

    def step(first):
        found = []
        for h in range(pack):
            d_e = jnp.concatenate([ref[first + h * half] for ref in d_refs], axis=0)
            found.append(diagonal(dot(left_mat, d_e, NN)))
        if pack == 1:
            result = found[0][0]
        else:
            straight = jnp.where(low, found[0][0], found[1][1])
            crossed = jnp.where(low, found[1][0], found[0][1])
            result = straight + pltpu.roll(crossed, columns, 1)
        right_sum[pl.ds(first, rows, stride=half), :] = result * (1.0 / rows)

    loop(half, step, left_mat.shape[1] <= MXU)
    count = kept_ref.shape[1]

    def part(place):
        return right_sum[pl.ds(pl.multiple_of(place * count, count), count), :]

    split_parts(part, "wide", kept_ref, sent_ref)


def forward_kernel(sizes, left_keys, right_keys, *refs):
    rows, channels, copies, groups, columns = sizes
    n_left, n_right = len(left_keys), len(right_keys)
    weight_ref, bias_ref, refs = refs[0], refs[1], refs[2:]
    left_refs, refs = list(zip(refs[:n_left], left_keys)), refs[n_left:]
    right_refs, refs = list(zip(refs[:n_right], right_keys)), refs[n_right:]
    out_ref, left_f32, right_f32, outer_t = refs
    place_right(right_refs, right_f32)
    left_t = place_left(left_refs, left_f32).T.astype(jnp.bfloat16)
    pack = LANES // columns
    half = channels // pack
    scale = 1.0 / rows
    bias = bias_ref[...]
    small = groups <= 8

    def e_step(start):
        diag = block_diagonal(right_f32, start, rows, channels, columns, copies)
        for h in range(pack):
            outer = (dot(left_t, diag[h], NN) * scale).astype(jnp.bfloat16)
            at = pl.ds((start + h * half) * channels, channels)
            for g in range(groups):
                outer_t[g, at, :] = outer[g * channels : (g + 1) * channels]

    loop(half, e_step, small)

    def g_step(g):
        pair = dot(weight_ref[...], outer_t[g], NN).T + bias
        pair = pair.astype(jnp.bfloat16)
        for n in range(copies):
            out_ref[n * groups + g] = pair[n * columns : (n + 1) * columns]

    loop(groups, g_step, small)


def add_kernel(kept, new, *outs):
    for n, out in enumerate(outs):
        out[...] = (kept[n] + new[n].astype(jnp.float32)).astype(out.dtype)


def last_kernel(n_left, n_right, inside, pairs, *refs):
    left_refs, refs = refs[:n_left], refs[n_left:]
    right_refs, refs = refs[:n_right], refs[n_right:]
    outs, (left_out, right_out, sent) = refs[:3], refs[3:]
    moves = [
        pltpu.make_async_copy(source, target, sent.at[n])
        for n, (source, target) in enumerate(zip((pairs, left_out, right_out), outs))
    ]
    moves[0].start()
    total = left_refs[0][...]
    for ref in left_refs[1:]:
        total = total + ref[...].astype(jnp.float32)
    if inside:
        total = jnp.concatenate([block_transpose(total[n]) for n in range(total.shape[0])], axis=0)
        left_out[...] = total.T.reshape(left_out.shape)
    else:
        left_out[...] = total
    moves[1].start()
    total = right_refs[0][...]
    for ref in right_refs[1:]:
        total = total + ref[...].astype(jnp.float32)
    rows, channels, columns = right_out.shape
    pack = LANES // columns
    half = channels // pack
    for s in range(rows):
        part = total[s * half : (s + 1) * half]
        for h in range(pack):
            right_out[s, h * half : (h + 1) * half, :] = part[:, h * columns : (h + 1) * columns]
    moves[2].start()
    for move in moves:
        move.wait()


def exchange(x, axis, m):
    size = lax.axis_size(axis)
    return lax.ppermute(x, axis, [(n, n ^ m) for n in range(size)])


def powers(size):
    return [1 << n for n in range(size.bit_length() - 1)]


def vmem(count):
    return [pl.BlockSpec(memory_space=pltpu.VMEM)] * count


def tile(left, right, out_weight, out_bias, cotangent):
    n_narrow, n_wide = lax.axis_size("narrow"), lax.axis_size("wide")
    part, channels, tile_rows = left.shape
    right_part, _, columns = right.shape
    width = cotangent.shape[2]
    rows = part * n_narrow
    copies = MXU // columns
    groups = tile_rows // copies
    pack = LANES // columns
    inside = part == groups and channels * part == MXU
    halves = 2
    count = groups // halves
    sizes = (rows, channels, copies, groups, columns)
    f32, bf16 = jnp.float32, jnp.bfloat16
    shape = jax.ShapeDtypeStruct
    work = channels * channels * tile_rows * columns
    limit = min(56 << 20, max(12 << 20, 3 * work))
    flops = 2 * work * width
    anywhere = pl.BlockSpec(memory_space=pl.ANY)
    outside = pl.BlockSpec(memory_space=pltpu.HBM)

    def call(kernel, outs, args, scratch=(), cost=0, in_specs=None, out_specs=None, **more):
        return pl.pallas_call(
            kernel,
            in_specs=in_specs or vmem(len(args)),
            out_specs=out_specs or vmem(len(outs)),
            out_shape=outs,
            scratch_shapes=scratch,
            compiler_params=pltpu.CompilerParams(vmem_limit_bytes=limit),
            cost_estimate=pl.CostEstimate(flops=cost, bytes_accessed=1 << 16, transcendentals=0),
            **more,
        )(*args)

    left_shape = (copies, part, groups * channels)
    right_shape = (right_part * channels // pack, LANES)

    hbm = functools.partial(pltpu.with_memory_space_constraint, memory_space=pltpu.HBM)

    steps = powers(n_wide)[:0:-1] + [1]
    narrow_steps = powers(n_narrow)[::-1]
    right_new = exchange(right, "wide", steps[0])
    source = left
    if not inside:
        source = left.reshape(part, channels, copies, groups).transpose(2, 0, 3, 1)
        source = source.reshape(left_shape)
    sources = [source, right, out_weight, cotangent]
    lefts, rights, weight, cot = call(
        functools.partial(prepare_kernel, inside),
        [shape((1,) + left_shape, bf16)] + [shape(v.shape, bf16) for v in sources[1:]],
        [hbm(v) for v in sources],
        [pltpu.VMEM(source.shape, bf16), pltpu.SemaphoreType.DMA((4,))],
        cost=flops // 16,
        in_specs=[outside] * 4,
    )
    by_e, transposed = call(
        weight_kernel,
        [shape((channels, channels, width), bf16), shape((width, channels * channels), bf16)],
        [weight],
        [pltpu.VMEM(weight.shape, f32)],
        cost=flops // 8,
    )

    def stack(one, other, change, after=()):
        total, shapes = 2 * one.shape[0], one.shape[1:]
        if change is dense:
            total, shapes = 2, right_shape
        args = [one, other, *after]
        specs = vmem(2) + [anywhere] * len(after)
        kernel = functools.partial(stack_kernel, change)
        return call(kernel, [shape((total,) + shapes, bf16)], args, in_specs=specs)[0]

    d_shape = shape((channels, count * channels, copies * columns), bf16)
    d_outer = []
    for n in range(halves):
        kernel = functools.partial(d_outer_kernel, sizes, n * count)
        d_outer += call(kernel, [d_shape], [cot, by_e], cost=flops // halves)

    keys = [0]
    for n, m in enumerate(steps):
        if n:
            right_new = exchange(rights, "wide", m)
        new = [k ^ m for k in keys]
        if n + 1 < len(steps):
            change = dense if n == 0 else None
            rights = stack(rights, right_new, change, d_outer[n : n + 1])
            keys = keys + new
    right_keys, rights = (keys, new), [rights, right_new]

    keys = [0]
    for n, m in enumerate(narrow_steps):
        left_new = exchange(lefts, "narrow", m)
        new = [k ^ m for k in keys]
        if n + 1 < len(narrow_steps):
            lefts = stack(lefts, left_new, None)
            keys = keys + new
    left_keys, lefts = (keys, new), [lefts, left_new]

    left_f32 = pltpu.VMEM((copies, n_narrow, part, groups * channels), f32)
    right_f32 = pltpu.VMEM((rows * channels // pack, LANES), f32)
    far, near = n_narrow // 2, n_wide // 2
    left_kept, left_sent = call(
        functools.partial(left_gradient_kernel, sizes, right_keys),
        [shape((far,) + left_shape, f32), shape((far,) + left_shape, bf16)],
        [*rights, *d_outer],
        [left_f32, right_f32, pltpu.VMEM((groups * channels, copies * rows), f32)],
        cost=flops,
    )
    right_kept, right_sent = call(
        functools.partial(right_gradient_kernel, sizes, left_keys),
        [shape((near,) + right_shape, f32), shape((near,) + right_shape, bf16)],
        [*lefts, *d_outer],
        [left_f32, right_f32],
        cost=flops,
    )
    left_new = exchange(left_sent, "narrow", 1)
    right_new = exchange(right_sent, "wide", 1)

    def add(kept, new):
        outs = [shape(kept.shape[1:], bf16 if n else f32) for n in range(kept.shape[0])]
        return list(call(add_kernel, outs, [kept, new]))

    right_sums = add(right_kept, right_new)
    for n in range(1, near):
        right_sums[n] = exchange(right_sums[n], "wide", 2 * n)
    left_sums = add(left_kept, left_new)
    for n in range(1, far):
        left_sums[n] = exchange(left_sums[n], "narrow", 2 * n)

    (pairs,) = call(
        functools.partial(forward_kernel, sizes, left_keys, right_keys),
        [shape(cotangent.shape, bf16)],
        [transposed, out_bias.reshape(1, width), *lefts, *rights],
        [left_f32, right_f32, pltpu.VMEM((groups, channels * channels, copies * columns), bf16)],
        cost=2 * flops,
    )
    last = [
        shape(cotangent.shape, bf16),
        shape((part, channels, tile_rows) if inside else left_shape, f32),
        shape((right_part, channels, columns), f32),
    ]
    pair_update, grad_left, grad_right = call(
        functools.partial(last_kernel, far, near, inside),
        last,
        [pairs, *left_sums, *right_sums],
        [pltpu.VMEM(v.shape, f32) for v in last[1:]] + [pltpu.SemaphoreType.DMA((3,))],
        out_specs=[outside] * 3,
    )
    if not inside:
        grad_left = grad_left.reshape(copies, part, groups, channels).transpose(1, 3, 0, 2)
        grad_left = grad_left.reshape(part, channels, tile_rows)
    return pair_update, grad_left, grad_right


def solution(mesh):
    return jax.shard_map(
        tile,
        mesh=mesh,
        in_specs=(
            P("narrow", None, "wide"),
            P("wide", None, "narrow"),
            P(),
            P(),
            P("wide", "narrow", None),
        ),
        out_specs=(P("wide", "narrow", None), P("narrow", None, "wide"), P("wide", None, "narrow")),
        check_vma=False,
    )
```

```python
import functools

import jax
import jax.numpy as jnp
from jax import lax
from jax.experimental import pallas as pl
from jax.experimental.pallas import tpu as pltpu
from jax.sharding import PartitionSpec as P


LANES = 128
MXU = 256
NT = (((1,), (1,)), ((), ()))
NN = (((1,), (0,)), ((), ()))


def dot(a, b, dims):
    return lax.dot_general(a, b, dims, preferred_element_type=jnp.float32)


def loop(count, body, small):
    if small:
        for n in range(count):
            body(n)
    else:
        lax.fori_loop(0, count, lambda n, c: (body(n), c)[1], 0)


def block_transpose(tile):
    size, lanes = tile.shape
    width = lanes // size
    row = lax.broadcasted_iota(jnp.int32, tile.shape, 0)
    block = lax.broadcasted_iota(jnp.int32, tile.shape, 1) // width
    result = tile
    for d in range(1, size):
        moved = pltpu.roll(pltpu.roll(tile, size - d, 0), width * d, 1)
        result = jnp.where(block == (row + d) % size, moved, result)
    return result


def block_diagonal(right_f32, first, rows, channels, columns, copies):
    pack = LANES // columns
    here = right_f32[pl.ds(first, rows, stride=channels // pack), :]
    lane = lax.broadcasted_iota(jnp.int32, here.shape, 1) // columns
    zero = jnp.zeros_like(here)
    moved = [here] + [pltpu.roll(here, n * columns, 1) for n in range(1, pack)]
    found = []
    for h in range(pack):
        blocks = []
        for n in range(copies):
            part = jnp.where(lane == n % pack, moved[(n - h) % pack], zero)
            tiles = [part if t == n // pack else zero for t in range(copies // pack)]
            blocks.append(jnp.concatenate(tiles, axis=1))
        found.append(jnp.concatenate(blocks, axis=0).astype(jnp.bfloat16))
    return found


def place_right(right_refs, right_f32):
    place = lax.axis_index("wide")
    for ref, keys in right_refs:
        rows = ref.shape[1]
        for n, key in enumerate(keys):
            start = pl.multiple_of((place ^ key) * rows, rows)
            right_f32[pl.ds(start, rows), :] = ref[n].astype(jnp.float32)


def place_left(left_refs, left_f32):
    place = lax.axis_index("narrow")
    for ref, keys in left_refs:
        for n, key in enumerate(keys):
            for copy in range(ref.shape[1]):
                left_f32[copy, place ^ key] = ref[n, copy].astype(jnp.float32)
    copies, places, part, lanes = left_f32.shape
    return left_f32[...].reshape(copies * places * part, lanes)


def dense(ref, out):
    rows, channels, columns = ref.shape
    pack = LANES // columns
    half = channels // pack
    for s in range(rows):
        block = ref[s].astype(jnp.float32)
        block = [block[h * half : (h + 1) * half] for h in range(pack)]
        out[s * half : (s + 1) * half, :] = jnp.concatenate(block, axis=1).astype(out.dtype)


def left_layout(ref, out):
    part, channels, tile_rows = ref.shape
    flat = ref[...].astype(jnp.float32).reshape(part * channels, tile_rows).T
    for n in range(out.shape[0]):
        out[n] = block_transpose(flat[n * part : (n + 1) * part]).astype(out.dtype)


def prepare_kernel(inside, *refs):
    sources, (left_out, *outs), (left_ref, sent) = refs[:4], refs[4:8], refs[8:]
    moves = [
        pltpu.make_async_copy(source, target, sent.at[n])
        for n, (source, target) in enumerate(zip(sources, [left_ref] + outs))
    ]
    for move in moves:
        move.start()
    moves[0].wait()
    if inside:
        left_layout(left_ref, left_out.at[0])
    else:
        left_out[0] = left_ref[...]
    for move in moves[1:]:
        move.wait()


def weight_kernel(weight_ref, by_e_ref, transposed_ref, weight_f32):
    channels = by_e_ref.shape[0]
    weight_f32[...] = weight_ref[...].astype(jnp.float32)
    for e in range(channels):
        by_e_ref[e] = weight_f32[pl.ds(e, channels, stride=channels), :].astype(jnp.bfloat16)
    flat = by_e_ref[...].reshape(channels * channels, weight_ref.shape[1])
    transposed_ref[...] = flat.astype(jnp.float32).T.astype(jnp.bfloat16)


def stack_kernel(change, one, other, *refs):
    out = refs[-1]
    count = out.shape[0] // 2
    if change is dense:
        dense(one, out.at[0])
        dense(other, out.at[1])
    else:
        out[:count] = one[...]
        out[count:] = other[...]


def d_outer_kernel(sizes, first, cot_ref, weight_ref, d_ref):
    _, channels, copies, groups, _ = sizes
    count = d_ref.shape[1] // channels
    per_dot = min(channels, MXU // channels)

    def step(g):
        slab = [cot_ref[n * groups + first + g] for n in range(copies)]
        slab = jnp.concatenate(slab, axis=0)
        for start in range(0, channels, per_dot):
            weight = weight_ref[start : start + per_dot].reshape(per_dot * channels, -1)
            piece = dot(weight, slab, NT).astype(jnp.bfloat16)
            for e in range(per_dot):
                at = pl.ds(g * channels, channels)
                d_ref[start + e, at, :] = piece[e * channels : (e + 1) * channels]

    loop(count, step, count <= 8)


def split_parts(total, axis, kept_ref, sent_ref):
    place = lax.axis_index(axis)
    count = kept_ref.shape[0]
    for n in range(count):
        keys = (n, n + count) if axis == "narrow" else (2 * n, 2 * n + 1)
        kept_ref[n] = total(place ^ keys[0]).astype(kept_ref.dtype)
        sent_ref[n] = total(place ^ keys[1]).astype(sent_ref.dtype)


def left_gradient_kernel(sizes, right_keys, *refs):
    rows, channels, copies, groups, columns = sizes
    n_right = len(right_keys)
    right_refs, refs = list(zip(refs[:n_right], right_keys)), refs[n_right:]
    d_refs, (kept_ref, sent_ref, left_f32, right_f32, left_sum) = refs[:-5], refs[-5:]
    place_right(right_refs, right_f32)
    pack = LANES // columns
    half = channels // pack
    small = groups * channels <= MXU
    if not small:
        left_sum[...] = jnp.zeros_like(left_sum)
    totals = []

    def step(first):
        diag = block_diagonal(right_f32, first, rows, channels, columns, copies)
        for h in range(pack):
            d_e = jnp.concatenate([ref[first + h * half] for ref in d_refs], axis=0)
            term = dot(d_e, diag[h], NT)
            if small:
                totals.append(term)
            else:
                left_sum[...] += term

    loop(half, step, small)
    if small:
        total = totals[0]
        for term in totals[1:]:
            total = total + term
    else:
        total = left_sum[...]
    left_f32[...] = (total.T * (1.0 / rows)).reshape(left_f32.shape)
    split_parts(lambda place: left_f32[:, place], "narrow", kept_ref, sent_ref)


def right_gradient_kernel(sizes, left_keys, *refs):
    rows, channels, copies, _, columns = sizes
    n_left = len(left_keys)
    left_refs, refs = list(zip(refs[:n_left], left_keys)), refs[n_left:]
    d_refs, (kept_ref, sent_ref, left_f32, right_sum) = refs[:-4], refs[-4:]
    left_mat = place_left(left_refs, left_f32).astype(jnp.bfloat16)
    pack = LANES // columns
    half = channels // pack
    low = lax.broadcasted_iota(jnp.int32, (rows, LANES), 1) < columns

    def diagonal(outer):
        found = []
        for h in range(pack):
            total = None
            for t in range(copies // pack):
                n = t * pack + h
                piece = outer[n * rows : (n + 1) * rows, t * LANES : (t + 1) * LANES]
                total = piece if total is None else total + piece
            found.append(total)
        return found

    def step(first):
        found = []
        for h in range(pack):
            d_e = jnp.concatenate([ref[first + h * half] for ref in d_refs], axis=0)
            found.append(diagonal(dot(left_mat, d_e, NN)))
        if pack == 1:
            result = found[0][0]
        else:
            straight = jnp.where(low, found[0][0], found[1][1])
            crossed = jnp.where(low, found[1][0], found[0][1])
            result = straight + pltpu.roll(crossed, columns, 1)
        right_sum[pl.ds(first, rows, stride=half), :] = result * (1.0 / rows)

    loop(half, step, left_mat.shape[1] <= MXU)
    count = kept_ref.shape[1]

    def part(place):
        return right_sum[pl.ds(pl.multiple_of(place * count, count), count), :]

    split_parts(part, "wide", kept_ref, sent_ref)


def forward_kernel(sizes, left_keys, right_keys, *refs):
    rows, channels, copies, groups, columns = sizes
    n_left, n_right = len(left_keys), len(right_keys)
    weight_ref, bias_ref, refs = refs[0], refs[1], refs[2:]
    left_refs, refs = list(zip(refs[:n_left], left_keys)), refs[n_left:]
    right_refs, refs = list(zip(refs[:n_right], right_keys)), refs[n_right:]
    out_ref, left_f32, right_f32, outer_t = refs
    place_right(right_refs, right_f32)
    left_t = place_left(left_refs, left_f32).T.astype(jnp.bfloat16)
    pack = LANES // columns
    half = channels // pack
    scale = 1.0 / rows
    bias = bias_ref[...]
    small = groups <= 8

    def e_step(start):
        diag = block_diagonal(right_f32, start, rows, channels, columns, copies)
        for h in range(pack):
            outer = (dot(left_t, diag[h], NN) * scale).astype(jnp.bfloat16)
            at = pl.ds((start + h * half) * channels, channels)
            for g in range(groups):
                outer_t[g, at, :] = outer[g * channels : (g + 1) * channels]

    loop(half, e_step, small)

    def g_step(g):
        pair = dot(weight_ref[...], outer_t[g], NN).T + bias
        pair = pair.astype(jnp.bfloat16)
        for n in range(copies):
            out_ref[n * groups + g] = pair[n * columns : (n + 1) * columns]

    loop(groups, g_step, small)


def add_kernel(kept, new, *outs):
    for n, out in enumerate(outs):
        out[...] = (kept[n] + new[n].astype(jnp.float32)).astype(out.dtype)


def last_kernel(n_left, n_right, inside, pairs, *refs):
    left_refs, refs = refs[:n_left], refs[n_left:]
    right_refs, refs = refs[:n_right], refs[n_right:]
    outs, (left_out, right_out, sent) = refs[:3], refs[3:]
    moves = [
        pltpu.make_async_copy(source, target, sent.at[n])
        for n, (source, target) in enumerate(zip((pairs, left_out, right_out), outs))
    ]
    moves[0].start()
    total = left_refs[0][...]
    for ref in left_refs[1:]:
        total = total + ref[...].astype(jnp.float32)
    if inside:
        total = jnp.concatenate([block_transpose(total[n]) for n in range(total.shape[0])], axis=0)
        left_out[...] = total.T.reshape(left_out.shape)
    else:
        left_out[...] = total
    moves[1].start()
    total = right_refs[0][...]
    for ref in right_refs[1:]:
        total = total + ref[...].astype(jnp.float32)
    rows, channels, columns = right_out.shape
    pack = LANES // columns
    half = channels // pack
    for s in range(rows):
        part = total[s * half : (s + 1) * half]
        for h in range(pack):
            right_out[s, h * half : (h + 1) * half, :] = part[:, h * columns : (h + 1) * columns]
    moves[2].start()
    for move in moves:
        move.wait()


def exchange(x, axis, m):
    size = lax.axis_size(axis)
    return lax.ppermute(x, axis, [(n, n ^ m) for n in range(size)])


def powers(size):
    return [1 << n for n in range(size.bit_length() - 1)]


def vmem(count):
    return [pl.BlockSpec(memory_space=pltpu.VMEM)] * count


def tile(left, right, out_weight, out_bias, cotangent):
    n_narrow, n_wide = lax.axis_size("narrow"), lax.axis_size("wide")
    part, channels, tile_rows = left.shape
    right_part, _, columns = right.shape
    width = cotangent.shape[2]
    rows = part * n_narrow
    copies = MXU // columns
    groups = tile_rows // copies
    pack = LANES // columns
    inside = part == groups and channels * part == MXU
    halves = 2
    count = groups // halves
    sizes = (rows, channels, copies, groups, columns)
    f32, bf16 = jnp.float32, jnp.bfloat16
    shape = jax.ShapeDtypeStruct
    work = channels * channels * tile_rows * columns
    limit = min(56 << 20, max(12 << 20, 3 * work))
    flops = 2 * work * width
    anywhere = pl.BlockSpec(memory_space=pl.ANY)
    outside = pl.BlockSpec(memory_space=pltpu.HBM)

    def call(kernel, outs, args, scratch=(), cost=0, in_specs=None, out_specs=None, **more):
        return pl.pallas_call(
            kernel,
            in_specs=in_specs or vmem(len(args)),
            out_specs=out_specs or vmem(len(outs)),
            out_shape=outs,
            scratch_shapes=scratch,
            compiler_params=pltpu.CompilerParams(vmem_limit_bytes=limit),
            cost_estimate=pl.CostEstimate(flops=cost, bytes_accessed=1 << 16, transcendentals=0),
            **more,
        )(*args)

    left_shape = (copies, part, groups * channels)
    right_shape = (right_part * channels // pack, LANES)

    hbm = functools.partial(pltpu.with_memory_space_constraint, memory_space=pltpu.HBM)

    steps = powers(n_wide)[:0:-1] + [1]
    narrow_steps = powers(n_narrow)[::-1]
    right_new = exchange(right, "wide", steps[0])
    source = left
    if not inside:
        source = left.reshape(part, channels, copies, groups).transpose(2, 0, 3, 1)
        source = source.reshape(left_shape)
    sources = [source, right, out_weight, cotangent]
    lefts, rights, weight, cot = call(
        functools.partial(prepare_kernel, inside),
        [shape((1,) + left_shape, bf16)] + [shape(v.shape, bf16) for v in sources[1:]],
        [hbm(v) for v in sources],
        [pltpu.VMEM(source.shape, bf16), pltpu.SemaphoreType.DMA((4,))],
        cost=flops // 16,
        in_specs=[outside] * 4,
    )
    by_e, transposed = call(
        weight_kernel,
        [shape((channels, channels, width), bf16), shape((width, channels * channels), bf16)],
        [weight],
        [pltpu.VMEM(weight.shape, f32)],
        cost=flops // 8,
    )

    def stack(one, other, change, after=()):
        total, shapes = 2 * one.shape[0], one.shape[1:]
        if change is dense:
            total, shapes = 2, right_shape
        args = [one, other, *after]
        specs = vmem(2) + [anywhere] * len(after)
        kernel = functools.partial(stack_kernel, change)
        return call(kernel, [shape((total,) + shapes, bf16)], args, in_specs=specs)[0]

    d_shape = shape((channels, count * channels, copies * columns), bf16)
    d_outer = []
    for n in range(halves):
        kernel = functools.partial(d_outer_kernel, sizes, n * count)
        d_outer += call(kernel, [d_shape], [cot, by_e], cost=flops // halves)

    keys = [0]
    for n, m in enumerate(steps):
        if n:
            right_new = exchange(rights, "wide", m)
        new = [k ^ m for k in keys]
        if n + 1 < len(steps):
            change = dense if n == 0 else None
            rights = stack(rights, right_new, change, d_outer[:1])
            keys = keys + new
    right_keys, rights = (keys, new), [rights, right_new]

    keys = [0]
    for n, m in enumerate(narrow_steps):
        left_new = exchange(lefts, "narrow", m)
        new = [k ^ m for k in keys]
        if n + 1 < len(narrow_steps):
            lefts = stack(lefts, left_new, None)
            keys = keys + new
    left_keys, lefts = (keys, new), [lefts, left_new]

    left_f32 = pltpu.VMEM((copies, n_narrow, part, groups * channels), f32)
    right_f32 = pltpu.VMEM((rows * channels // pack, LANES), f32)
    far, near = n_narrow // 2, n_wide // 2
    left_kept, left_sent = call(
        functools.partial(left_gradient_kernel, sizes, right_keys),
        [shape((far,) + left_shape, f32), shape((far,) + left_shape, bf16)],
        [*rights, *d_outer],
        [left_f32, right_f32, pltpu.VMEM((groups * channels, copies * rows), f32)],
        cost=flops,
    )
    right_kept, right_sent = call(
        functools.partial(right_gradient_kernel, sizes, left_keys),
        [shape((near,) + right_shape, f32), shape((near,) + right_shape, bf16)],
        [*lefts, *d_outer],
        [left_f32, right_f32],
        cost=flops,
    )
    left_new = exchange(left_sent, "narrow", far)
    right_new = exchange(right_sent, "wide", 1)

    def add(kept, new):
        outs = [shape(kept.shape[1:], bf16 if n else f32) for n in range(kept.shape[0])]
        return list(call(add_kernel, outs, [kept, new]))

    right_sums = add(right_kept, right_new)
    for n in range(1, near):
        right_sums[n] = exchange(right_sums[n], "wide", 2 * n)
    left_sums = add(left_kept, left_new)
    for n in range(1, far):
        left_sums[n] = exchange(left_sums[n], "narrow", n)

    (pairs,) = call(
        functools.partial(forward_kernel, sizes, left_keys, right_keys),
        [shape(cotangent.shape, bf16)],
        [transposed, out_bias.reshape(1, width), *lefts, *rights],
        [left_f32, right_f32, pltpu.VMEM((groups, channels * channels, copies * columns), bf16)],
        cost=2 * flops,
    )
    last = [
        shape(cotangent.shape, bf16),
        shape((part, channels, tile_rows) if inside else left_shape, f32),
        shape((right_part, channels, columns), f32),
    ]
    pair_update, grad_left, grad_right = call(
        functools.partial(last_kernel, far, near, inside),
        last,
        [pairs, *left_sums, *right_sums],
        [pltpu.VMEM(v.shape, f32) for v in last[1:]] + [pltpu.SemaphoreType.DMA((3,))],
        out_specs=[outside] * 3,
    )
    if not inside:
        grad_left = grad_left.reshape(copies, part, groups, channels).transpose(1, 3, 0, 2)
        grad_left = grad_left.reshape(part, channels, tile_rows)
    return pair_update, grad_left, grad_right


def solution(mesh):
    return jax.shard_map(
        tile,
        mesh=mesh,
        in_specs=(
            P("narrow", None, "wide"),
            P("wide", None, "narrow"),
            P(),
            P(),
            P("wide", "narrow", None),
        ),
        out_specs=(P("wide", "narrow", None), P("narrow", None, "wide"), P("wide", None, "narrow")),
        check_vma=False,
    )
```
